32 devices in a mesh: dp: 4 (over z), ep: 8 (over y, x, core).
Axes of the slice: x: 2, y: 2, z: 4, core: 2. Of those that a mesh axis runs over, the one named last changes fastest.
Arguments:
- x_norm: bfloat16 [8192, 4096], P(('dp', 'ep'))
- route_idx: int32 [8192, 2], P(('dp', 'ep'))
- w_router: bfloat16 [4096, 8], replicated
- w_gate: bfloat16 [8, 4096, 1376], P('ep')
- w_up: bfloat16 [8, 4096, 1376], P('ep')
- w_down: bfloat16 [8, 1376, 4096], P('ep')
- grad_out: bfloat16 [8192, 4096], P(('dp', 'ep'))
Outputs:
- output 1: bfloat16 [8192, 4096], P(('dp', 'ep'))
- output 2: float32 [8, 4096, 1376], P('ep')
- output 3: float32 [8, 4096, 1376], P('ep')
- output 4: float32 [8, 1376, 4096], P('ep')
- output 5: float32 [4096, 8], replicated
All inputs are finite; a program needn't handle non-finite values.
Results may differ from the reference program's by a relative error of at most 0.00526722.
Values are sent between devices in bfloat16 or wider.
A program may use at most 1 GiB of HBM per device.

```python
import jax
import jax.numpy as jnp
from jax import lax

D = 4096
FF = 1376
EXPERTS = 8
TOP = 2
TOK_DEV = 256
SHARDS = 32
CAP = 192
TOKENS = SHARDS * TOK_DEV
N_CHOICE = TOKENS * TOP


def shuffle_rows(row_key):
    return jax.random.permutation(row_key, TOK_DEV)


def permute_rows(shard_rows, row_order):
    return shard_rows[row_order]


def draw_routes(route_key):
    perm_key, shift_key, order_key = jax.random.split(route_key, 3)
    expert_order = jax.random.permutation(perm_key, EXPERTS).astype(jnp.int32)
    shifts = jax.random.randint(shift_key, (SHARDS,), 0, EXPERTS - 1, dtype=jnp.int32)
    tok_pos = jnp.arange(TOK_DEV, dtype=jnp.int32)
    choice_pos = jnp.arange(TOP, dtype=jnp.int32)
    is_hot = tok_pos < CAP
    cycle_pos = (tok_pos * TOP - jnp.minimum(tok_pos, CAP))[:, None] + choice_pos[None, :] - is_hot[:, None].astype(jnp.int32)
    labels = 1 + (cycle_pos[None, :, :] + shifts[:, None, None]) % (EXPERTS - 1)
    hot_slot = is_hot[:, None] & (choice_pos[None, :] == 0)
    labels = jnp.where(hot_slot[None, :, :], 0, labels)
    experts = expert_order[labels]
    row_orders = jax.vmap(shuffle_rows)(jax.random.split(order_key, SHARDS))
    experts = jax.vmap(permute_rows)(experts, row_orders)
    return experts.reshape(TOKENS, TOP).astype(jnp.int32)


def setup_inputs(seed: int = 0) -> dict:
    base_key = jax.random.key(seed)
    key_list = jax.random.split(base_key, 7)
    x_norm = jax.random.normal(key_list[0], (TOKENS, D), jnp.float32)
    w_router = jax.random.normal(key_list[2], (D, EXPERTS), jnp.float32) * D ** -0.5
    w_gate = jax.random.normal(key_list[3], (EXPERTS, D, FF), jnp.float32) * D ** -0.5
    w_up = jax.random.normal(key_list[4], (EXPERTS, D, FF), jnp.float32) * D ** -0.5
    w_down = jax.random.normal(key_list[5], (EXPERTS, FF, D), jnp.float32) * FF ** -0.5
    grad_out = jax.random.normal(key_list[6], (TOKENS, D), jnp.float32)
    return {
        "x_norm": x_norm.astype(jnp.bfloat16),
        "route_idx": draw_routes(key_list[1]),
        "w_router": w_router.astype(jnp.bfloat16),
        "w_gate": w_gate.astype(jnp.bfloat16),
        "w_up": w_up.astype(jnp.bfloat16),
        "w_down": w_down.astype(jnp.bfloat16),
        "grad_out": grad_out.astype(jnp.bfloat16),
    }


def expert_backward(x_rows, dy_rows, gate_rows, w_gate_e, w_up_e, w_down_e):
    z_gate = jnp.dot(x_rows, w_gate_e, preferred_element_type=jnp.float32)
    z_up = jnp.dot(x_rows, w_up_e, preferred_element_type=jnp.float32)
    sigmoid_z = jax.nn.sigmoid(z_gate)
    silu_z = z_gate * sigmoid_z
    act_rows = (silu_z * z_up).astype(jnp.bfloat16)
    out_rows = jnp.dot(act_rows, w_down_e, preferred_element_type=jnp.float32)
    dy_wide = dy_rows.astype(jnp.float32)
    dgate_rows = jnp.sum(out_rows * dy_wide, axis=1)
    d_out = (gate_rows[:, None] * dy_wide).astype(jnp.bfloat16)
    d_act = jnp.dot(d_out, w_down_e.T, preferred_element_type=jnp.float32)
    d_zgate = (d_act * z_up * sigmoid_z * (1.0 + z_gate * (1.0 - sigmoid_z))).astype(jnp.bfloat16)
    d_zup = (d_act * silu_z).astype(jnp.bfloat16)
    dx_rows = (jnp.dot(d_zgate, w_gate_e.T, preferred_element_type=jnp.float32) + jnp.dot(d_zup, w_up_e.T, preferred_element_type=jnp.float32)).astype(jnp.bfloat16)
    grad_gate = jnp.dot(x_rows.T, d_zgate, preferred_element_type=jnp.float32)
    grad_up = jnp.dot(x_rows.T, d_zup, preferred_element_type=jnp.float32)
    grad_down = jnp.dot(act_rows.T, d_out, preferred_element_type=jnp.float32)
    return dx_rows, dgate_rows, grad_gate, grad_up, grad_down


def reference(x_norm, route_idx, w_router, w_gate, w_up, w_down, grad_out):
    logits = jnp.dot(x_norm, w_router, preferred_element_type=jnp.float32)
    gate_probs = jax.nn.softmax(jnp.take_along_axis(logits, route_idx, axis=1), axis=-1)
    expert_ids = jnp.arange(EXPERTS, dtype=jnp.int32)
    shard_idx = route_idx.reshape(SHARDS, TOK_DEV * TOP)
    one_hot = (shard_idx[:, :, None] == expert_ids).astype(jnp.int32)
    rank_in = jnp.sum((jnp.cumsum(one_hot, axis=1) - one_hot) * one_hot, axis=2)
    slot_ids = (shard_idx * (SHARDS * CAP) + jnp.arange(SHARDS, dtype=jnp.int32)[:, None] * CAP + rank_in).reshape(N_CHOICE)
    slot_table = jnp.full((EXPERTS * SHARDS * CAP,), N_CHOICE, jnp.int32).at[slot_ids].set(jnp.arange(N_CHOICE, dtype=jnp.int32)).reshape(EXPERTS, SHARDS * CAP)
    gate_flat = gate_probs.reshape(N_CHOICE)

    def one_expert(operands):
        w_gate_e, w_up_e, w_down_e, choice_ids = operands
        is_valid = choice_ids < N_CHOICE
        safe_ids = jnp.minimum(choice_ids, N_CHOICE - 1)
        x_rows = jnp.where(is_valid[:, None], x_norm[safe_ids // TOP], 0.0)
        dy_rows = jnp.where(is_valid[:, None], grad_out[safe_ids // TOP], 0.0)
        gate_rows = jnp.where(is_valid, gate_flat[safe_ids], 0.0)
        return expert_backward(x_rows, dy_rows, gate_rows, w_gate_e, w_up_e, w_down_e)

    dx_rows, dgate_rows, grad_gate, grad_up, grad_down = lax.map(one_expert, (w_gate, w_up, w_down, slot_table))
    dx_choice = dx_rows.reshape(EXPERTS * SHARDS * CAP, D)[slot_ids].reshape(TOKENS, TOP, D)
    dgate = dgate_rows.reshape(EXPERTS * SHARDS * CAP)[slot_ids].reshape(TOKENS, TOP)
    d_sel = gate_probs * (dgate - jnp.sum(gate_probs * dgate, axis=1, keepdims=True))
    d_logits = jnp.sum(jnp.where(route_idx[:, :, None] == expert_ids, d_sel[:, :, None], 0.0), axis=1).astype(jnp.bfloat16)
    du_router = jnp.dot(d_logits, w_router.T, preferred_element_type=jnp.float32)
    grad_x = (jnp.sum(dx_choice.astype(jnp.float32), axis=1) + du_router).astype(jnp.bfloat16)
    grad_router = jnp.dot(x_norm.T, d_logits, preferred_element_type=jnp.float32)
    return grad_x, grad_gate, grad_up, grad_down, grad_router
```

```python
import functools

import jax
import jax.numpy as jnp
from jax import lax
from jax.experimental import pallas as pl
from jax.experimental.pallas import tpu as pltpu
from jax.sharding import PartitionSpec as P

BF = jnp.bfloat16
F32 = jnp.float32
MESH = pl.DeviceIdType.MESH
ANY = pl.BlockSpec(memory_space=pl.ANY)
NT = (((1,), (1,)), ((), ()))
TN = (((0,), (0,)), ((), ()))
NN = (((1,), (0,)), ((), ()))
VMEM_LIMIT = 67_000_000
NOWHERE = 300.0


def mm(left, right, dims=NN):
    return lax.dot_general(left, right, dims, preferred_element_type=F32)


def where_am_i():
    z = lax.axis_index("dp")
    e = lax.axis_index("ep")
    return z, e, e // 4, (e // 2) % 2, e % 2


def shard_of(z, y, x, c):
    return z * 8 + y * 4 + x * 2 + c


def other_levels(z):
    return z + 1 - 2 * (z % 2), 2 - z // 2, 3 - 3 * (z // 2)


class Shapes:
    def __init__(self, tokens, width, hidden, cap):
        self.t, self.d, self.f, self.cap = tokens, width, hidden, cap
        self.pair = 2 * cap
        self.wide = min(512, width)
        half = (hidden // 2 + 127) // 128 * 128
        self.cuts = [(0, half), (half, hidden)] if half < hidden else [(0, hidden)]


class Links:
    def __init__(self, bufs, own, ssem, rsem, partner):
        self.bufs, self.own, self.ssem, self.rsem, self.partner = bufs, own, ssem, rsem, partner
        self.sent = {}

    def _copy(self, slot, part, sid, dev, own):
        src = self.own[part] if own else self.bufs[part].at[sid]
        return pltpu.make_async_remote_copy(
            src_ref=src,
            dst_ref=self.bufs[part].at[sid],
            send_sem=self.ssem.at[slot, part],
            recv_sem=self.rsem.at[sid, part],
            device_id=dev,
            device_id_type=MESH,
        )

    def _do(self, when, go):
        if when is None:
            go()
        else:
            pl.when(when())(go)

    def send(self, tag, sid, dev, parts=(0, 1, 2), when=None, own=False):
        if tag not in self.sent:
            self.sent[tag] = (len(self.sent), sid, dev, parts, when, own)
        slot = self.sent[tag][0]

        def go():
            for part in parts:
                self._copy(slot, part, sid(), dev, own).start()

        self._do(when, go)

    def arrived(self, sid, parts=(0, 1, 2), when=None):
        def go():
            for part in parts:
                self._copy(0, part, sid(), self.partner, False).wait_recv()

        self._do(when, go)

    def drain(self):
        for slot, sid, dev, parts, when, own in self.sent.values():

            def go():
                for part in parts:
                    self._copy(slot, part, sid(), dev, own).wait_send()

            self._do(when, go)

    def along_column(self, name, step, z, shard, above, below):
        top, bottom = (lambda: shard(z + step)), (lambda: shard(z - step))
        has_top, has_bottom = (lambda: z + step <= 3), (lambda: z >= step)
        self.arrived(top, when=has_top)
        if step < 3:
            self.send((name, step, 0), top, below, when=lambda: jnp.logical_and(has_top(), z > 0))
        self.send((name, step, 1), top, self.partner, when=has_top)
        self.arrived(bottom, when=has_bottom)
        if step < 3:
            self.send((name, step, 2), bottom, above, when=lambda: jnp.logical_and(has_bottom(), z < 3))
        self.send((name, step, 3), bottom, self.partner, when=has_bottom)


def enter(z, peers, above, below):
    barrier = pltpu.get_barrier_semaphore()

    def greet(dev):
        pl.semaphore_signal(barrier, inc=1, device_id=dev, device_id_type=MESH)

    for dev in peers:
        greet(dev)

    @pl.when(z < 3)
    def _():
        greet(above)

    @pl.when(z > 0)
    def _():
        greet(below)

    pl.semaphore_wait(barrier, len(peers) + (5 - z) // 3 + (z + 2) // 3)


def load_weights(weights, w_vmem, w_sem):
    for k in range(3):
        pltpu.make_async_copy(weights[k], w_vmem.at[k], w_sem.at[k]).start()


def await_weights(weights, w_vmem, w_sem):
    for k in range(3):
        pltpu.make_async_copy(weights[k], w_vmem.at[k], w_sem.at[k]).wait()


def pick_rows(sh, half, stage, meta, expert, xs, do, gs):
    cap, t, wide = sh.cap, sh.t, sh.wide
    pos = meta[half, pl.ds(expert, 1), :]
    gate = meta[half, pl.ds(8 + expert, 1), :]
    slot = lax.broadcasted_iota(jnp.int32, (cap, t), 0).astype(F32)
    hit = slot == pos
    pick = jnp.where(hit, 1.0, 0.0).astype(BF)
    gate_col = jnp.sum(jnp.where(hit, gate, 0.0), axis=1, keepdims=True)
    rows = slice(half * cap, (half + 1) * cap)
    for n in range(0, sh.d, wide):
        cols = slice(n, n + wide)
        xs[rows, cols] = mm(pick, stage[2 * half, :, cols]).astype(BF)
        g_sel = mm(pick, stage[2 * half + 1, :, cols])
        do[rows, cols] = (gate_col * g_sel).astype(BF)
        if gs is not None:
            gs[rows, cols] = g_sel.astype(BF)


def expert_rows(sh, w, xs, do, a, d1, d3):
    for lo, hi in sh.cuts:
        cols = slice(lo, hi)
        z1 = mm(xs[...], w[0, cols, :], NT)
        z3 = mm(xs[...], w[1, cols, :], NT)
        da = mm(do[...], w[2, cols, :], NT)
        sig = jax.nn.sigmoid(z1)
        silu = z1 * sig
        a[:, cols] = (silu * z3).astype(BF)
        d1[:, cols] = (da * z3 * sig * (1.0 + z1 * (1.0 - sig))).astype(BF)
        d3[:, cols] = (da * silu).astype(BF)


def token_rows(sh, w, a, d1, d3, gs, q):
    acc = jnp.zeros((sh.pair, 1), F32)
    for n in range(0, sh.d, sh.wide):
        cols = slice(n, n + sh.wide)
        out = mm(a[...], w[2, :, cols])
        acc = acc + jnp.sum(out * gs[:, cols].astype(F32), axis=1, keepdims=True)
    q[...] = jnp.broadcast_to(acc, q.shape)
    for n in range(0, sh.d, sh.wide):
        cols = slice(n, n + sh.wide)
        row = mm(d1[...], w[0, :, cols]) + mm(d3[...], w[1, :, cols])
        gs[:, cols] = row.astype(BF)


class Rows:
    def __init__(self, sh, expert, bufs, own, w, vm, sems, hbm):
        self.sh, self.expert, self.bufs, self.own, self.w = sh, expert, bufs, own, w
        self.stage, self.meta, self.xs, self.do, self.a, self.d1, self.d3 = vm
        self.in_sem, self.out_sem = sems
        self.xs_h, self.do_h, self.d_h = hbm

    def _in(self, half, part, sid, own=False):
        src = self.own[part] if own else self.bufs[part].at[sid]
        dst = self.meta.at[half] if part == 2 else self.stage.at[2 * half + part]
        return pltpu.make_async_copy(src, dst, self.in_sem.at[half, part])

    def load(self, sids, own_first=None):
        for half in range(2):
            for part in (2, 0, 1):
                if half == 0 and own_first is not None:

                    @pl.when(own_first)
                    def _():
                        self._in(half, part, sids[half], True).start()

                    @pl.when(jnp.logical_not(own_first))
                    def _():
                        self._in(half, part, sids[half]).start()
                else:
                    self._in(half, part, sids[half]).start()

    def select(self, sids, gs=None):
        for half in range(2):
            for part in (2, 0, 1):
                self._in(half, part, sids[half]).wait()
            pick_rows(self.sh, half, self.stage, self.meta, self.expert, self.xs, self.do, gs)

    def _out(self, k, row0):
        at = pl.ds(row0, self.sh.pair)
        src = (self.xs, self.do, self.d1, self.d3, self.a)[k]
        dst = (self.xs_h, self.do_h)[k].at[at, :] if k < 2 else self.d_h.at[k - 2, at, :]
        return pltpu.make_async_copy(src, dst, self.out_sem.at[k])

    def forward(self, row0):
        for k in (0, 1):
            self._out(k, row0).start()
        expert_rows(self.sh, self.w, self.xs, self.do, self.a, self.d1, self.d3)
        for k in (2, 3, 4):
            self._out(k, row0).start()

    def finish(self, row0):
        for k in range(5):
            self._out(k, row0).wait()


def add_weight_grads(sh, rows, hbm, grad_in, put, vm, sems, tick=None):
    xs_h, do_h, d_h = hbm
    d_v, y_v, acc = vm
    d_sem, y_sem, i_sem, o_sem = sems
    nblk = sh.d // sh.wide
    total = 3 * nblk

    def d_copy(k):
        return pltpu.make_async_copy(d_h.at[k, pl.ds(0, rows), :], d_v.at[k % 2], d_sem.at[k % 2])

    def y_copy(it, slot, src):
        col = pl.multiple_of((it % nblk) * sh.wide, sh.wide)
        return pltpu.make_async_copy(src.at[pl.ds(0, rows), pl.ds(col, sh.wide)], y_v.at[slot], y_sem.at[slot])

    def y_start(it):
        @pl.when(it < 2 * nblk)
        def _():
            y_copy(it, it % 2, xs_h).start()

        @pl.when(it >= 2 * nblk)
        def _():
            y_copy(it, it % 2, do_h).start()

    def acc_in(it):
        col = pl.multiple_of((it % nblk) * sh.wide, sh.wide)
        return pltpu.make_async_copy(grad_in.at[it // nblk, :, pl.ds(col, sh.wide)], acc.at[it % 3], i_sem.at[it % 3])

    def acc_out(it, start):
        col = pl.multiple_of((it % nblk) * sh.wide, sh.wide)
        put(it // nblk, col, acc.at[it % 3], o_sem.at[it % 3], start)

    d_copy(0).start()
    y_start(0)
    if grad_in is not None:
        acc_in(0).start()

    def body(it, carry):
        k = it // nblk

        @pl.when(it % nblk == 0)
        def _():
            @pl.when(k < 2)
            def _():
                d_copy(k + 1).start()

            d_copy(k).wait()

        @pl.when(it + 1 < total)
        def _():
            y_start(it + 1)

        @pl.when(it >= 2)
        def _():
            acc_out(it - 2, False)

        if grad_in is not None:

            @pl.when(it + 1 < total)
            def _():
                acc_in(it + 1).start()

        if tick is not None:
            tick(it)
        y_copy(it, it % 2, xs_h).wait()
        if grad_in is not None:
            acc_in(it).wait()
            acc[it % 3] += mm(d_v[k % 2], y_v[it % 2], TN)
        else:
            acc[it % 3] = mm(d_v[k % 2], y_v[it % 2], TN)
        acc_out(it, True)
        return carry

    lax.fori_loop(0, total, body, None)
    acc_out(total - 2, False)
    acc_out(total - 1, False)


def put_stacked(grads):
    def put(k, col, src, sem, start):
        copy = pltpu.make_async_copy(src, grads.at[k, :, pl.ds(col, src.shape[-1])], sem)
        copy.start() if start else copy.wait()

    return put


def put_separate(grads):
    def put(k, col, src, sem, start):
        if start:
            for j in range(3):

                @pl.when(k == j)
                def _():
                    pltpu.make_async_copy(src, grads[j].at[:, pl.ds(col, src.shape[-1])], sem).start()
        else:
            pltpu.make_async_copy(src, grads[0].at[:, pl.ds(col, src.shape[-1])], sem).wait()

    return put


def row_scratch(sh):
    return (
        pltpu.VMEM((3, sh.f, sh.d), BF),
        pltpu.VMEM((4, sh.t, sh.d), BF),
        pltpu.VMEM((2, 16, sh.t), F32),
        pltpu.VMEM((sh.pair, sh.d), BF),
        pltpu.VMEM((sh.pair, sh.d), BF),
        pltpu.VMEM((sh.pair, sh.f), BF),
        pltpu.VMEM((sh.pair, sh.f), BF),
        pltpu.VMEM((sh.pair, sh.f), BF),
    )


def grad_scratch(sh, rows):
    return (
        pltpu.VMEM((2, rows, sh.f), BF),
        pltpu.VMEM((2, rows, sh.wide), BF),
        pltpu.VMEM((3, sh.f, sh.wide), F32),
    )


GRAD_SEMS = [pltpu.SemaphoreType.DMA((2,)), pltpu.SemaphoreType.DMA((2,)), pltpu.SemaphoreType.DMA((3,)), pltpu.SemaphoreType.DMA((3,))]
ROW_SEMS = [pltpu.SemaphoreType.DMA((3,)), pltpu.SemaphoreType.DMA((2, 3)), pltpu.SemaphoreType.DMA((5,))]


def first_kernel(sh, x_in, g_in, m_in, w1, w3, w2, xb, gb, mb, rback, qback, r_h, q_h, xs_h, do_h, d_h, grads,
                 ssem, rsem, ret_s, ret_r, w_sem, in_sem, out_sem, loc_sem, *grad_sems):
    z, e, y, x, c = where_am_i()
    me = shard_of(z, y, x, c)
    bufs, own, weights = (xb, gb, mb), (x_in, g_in, m_in), (w1, w3, w2)
    partner, xn, yn = (z, e + 1 - 2 * c), (z, e + 2 - 4 * x), (z, e + 4 - 8 * y)
    above, below = (z + 1, e), (z - 1, e)
    links = Links(bufs, own, ssem, rsem, partner)
    column = [(y, x), (y, 1 - x), (1 - y, x), (1 - y, 1 - x)]
    mine = [shard_of(z, yy, xx, c) for yy, xx in column]
    theirs = [shard_of(z, yy, xx, 1 - c) for yy, xx in column]
    plane = [(z, yy * 4 + xx * 2 + cc) for yy, xx in column for cc in (c, 1 - c)]

    enter(z, plane[1:], above, below)
    links.send("p", lambda: me, partner, own=True)
    links.send("x", lambda: me, xn, own=True)
    links.send("y", lambda: me, yn, own=True)
    links.send("u", lambda: me, above, when=lambda: z < 3, own=True)
    links.send("d", lambda: me, below, when=lambda: z > 0, own=True)

    def line(step):
        links.along_column("o", step, z, lambda lev: shard_of(lev, y, x, c), above, below)

    def ret(k):
        for part, (src, dst) in enumerate(((r_h, rback), (q_h, qback))):
            yield pltpu.make_async_remote_copy(
                src_ref=src.at[k], dst_ref=dst.at[e], send_sem=ret_s.at[k, part], recv_sem=ret_r.at[e, part],
                device_id=plane[k], device_id_type=MESH)

    def ret_in(k):
        peer = plane[k][1]
        for part, (src, dst) in enumerate(((r_h, rback), (q_h, qback))):
            yield pltpu.make_async_remote_copy(
                src_ref=src.at[k], dst_ref=dst.at[peer], send_sem=ret_s.at[k, part], recv_sem=ret_r.at[peer, part],
                device_id=plane[k], device_id_type=MESH)

    def rows_phase(w, stage, meta, xs, do, a, d1, d3, gs, q, qt):
        load_weights(weights, w, w_sem)
        rows = Rows(sh, e, bufs, own, w, (stage, meta, xs, do, a, d1, d3), (in_sem, out_sem), (xs_h, do_h, d_h))

        def body(p, carry):
            @pl.when(p == 0)
            def _():
                links.arrived(lambda: theirs[0])

            @pl.when(p == 1)
            def _():
                links.arrived(lambda: mine[1])
                links.send("xy", lambda: mine[1], yn, parts=(1,))
                links.send("xp", lambda: mine[1], partner)
                links.arrived(lambda: mine[2])
                links.send("yx", lambda: mine[2], xn, parts=(0, 2))
                links.send("yp", lambda: mine[2], partner)
                line(1)
                links.arrived(lambda: theirs[1])

            @pl.when(p == 2)
            def _():
                links.arrived(lambda: theirs[2])

            @pl.when(p == 3)
            def _():
                links.arrived(lambda: mine[3])
                links.send("dp", lambda: mine[3], partner)
                links.arrived(lambda: theirs[3])

            yy = y + p // 2 - 2 * y * (p // 2)
            xx = x + p % 2 - 2 * x * (p % 2)
            sids = (shard_of(z, yy, xx, c), shard_of(z, yy, xx, 1 - c))
            row0 = pl.multiple_of(p * sh.pair, sh.pair)
            rows.load(sids, own_first=p == 0)
            rows.select(sids, gs)

            @pl.when(p == 0)
            def _():
                await_weights(weights, w, w_sem)

            rows.forward(row0)
            token_rows(sh, w, a, d1, d3, gs, q)
            qt[...] = jnp.transpose(q[...])[0:8, :]
            for half in range(2):
                at = slice(half * sh.cap, (half + 1) * sh.cap)

                @pl.when(p * 2 + half == 0)
                def _():
                    pltpu.make_async_copy(gs.at[at, :], rback.at[e], loc_sem.at[half]).start()
                    pltpu.make_async_copy(qt, qback.at[e], loc_sem.at[2 + half]).start()

                @pl.when(p * 2 + half > 0)
                def _():
                    pltpu.make_async_copy(gs.at[at, :], r_h.at[p * 2 + half], loc_sem.at[half]).start()
                    pltpu.make_async_copy(qt, q_h.at[p * 2 + half], loc_sem.at[2 + half]).start()

            for half in range(2):
                at = slice(half * sh.cap, (half + 1) * sh.cap)
                pltpu.make_async_copy(gs.at[at, :], r_h.at[p * 2 + half], loc_sem.at[half]).wait()
                pltpu.make_async_copy(qt, q_h.at[p * 2 + half], loc_sem.at[2 + half]).wait()
            for k in range(1, 8):

                @pl.when(p == k // 2)
                def _():
                    for copy in ret(k):
                        copy.start()

            rows.finish(row0)
            return carry

        lax.fori_loop(0, 4, body, None)

    pl.run_scoped(rows_phase, *row_scratch(sh), pltpu.VMEM((sh.pair, sh.d), BF), pltpu.VMEM((sh.pair, 128), F32),
                  pltpu.VMEM((8, sh.pair), F32))

    def tick(it):
        @pl.when(it == 1)
        def _():
            line(2)

    def grads_phase(*vm):
        add_weight_grads(sh, 4 * sh.pair, (xs_h, do_h, d_h), None, put_stacked(grads), vm, grad_sems, tick)

    pl.run_scoped(grads_phase, *grad_scratch(sh, 4 * sh.pair))
    line(3)
    for step in (1, 2, 3):
        links.arrived(lambda: shard_of(z + step, y, x, 1 - c), when=lambda: z + step <= 3)
        links.arrived(lambda: shard_of(z - step, y, x, 1 - c), when=lambda: z >= step)
    for k in range(1, 8):
        for copy in ret(k):
            copy.wait_send()
        for copy in ret_in(k):
            copy.wait_recv()
    links.drain()


def second_kernel(sh, xb_in, gb_in, mb_in, grads_in, w1, w3, w2, xb, gb, mb, grads, xs_h, do_h, d_h,
                  ssem, rsem, w_sem, in_sem, out_sem, *grad_sems):
    z, e, y, x, c = where_am_i()
    bufs, weights = (xb, gb, mb), (w1, w3, w2)
    partner, xn, yn = (z, e + 1 - 2 * c), (z, e + 2 - 4 * x), (z, e + 4 - 8 * y)
    above, below = (z + 1, e), (z - 1, e)
    links = Links(bufs, None, ssem, rsem, partner)
    levels = other_levels(z)
    f1, f2, f3 = levels

    enter(z, (partner, xn, yn), above, below)
    sides = ((y, 1 - x), (1 - y, x))

    def diag(lev):
        return shard_of(lev, 1 - y, 1 - x, c)

    links.send("u", lambda: diag(z), above, when=lambda: z < 3)
    links.send("d", lambda: diag(z), below, when=lambda: z > 0)
    for k in range(3):
        links.send(("x", k), lambda k=k: shard_of(levels[k], y, x, c), xn)
        links.send(("y", k), lambda k=k: shard_of(levels[k], y, x, c), yn)

    def stage(step):
        lev = levels[step - 1]
        for k, (yy, xx) in enumerate(sides):
            links.arrived(lambda: shard_of(lev, yy, xx, c))
            links.send(("p", step, k), lambda yy=yy, xx=xx: shard_of(lev, yy, xx, c), partner)
        links.along_column("d", step, z, diag, above, below)

    def theirs(step):
        lev = levels[step - 1]
        for yy, xx in sides:
            links.arrived(lambda: shard_of(lev, yy, xx, 1 - c))
        links.arrived(lambda: shard_of(z + step, 1 - y, 1 - x, 1 - c), when=lambda: z + step <= 3)
        links.arrived(lambda: shard_of(z - step, 1 - y, 1 - x, 1 - c), when=lambda: z >= step)

    hbm = (xs_h, do_h, d_h)
    blocks = 3 * (sh.d // sh.wide)

    def group(f, carry):
        def rows_phase(w, stage_v, meta, xs, do, a, d1, d3):
            load_weights(weights, w, w_sem)
            rows = Rows(sh, e, bufs, None, w, (stage_v, meta, xs, do, a, d1, d3), (in_sem, out_sem), hbm)

            def body(i, carry):
                first = (3 - f) // 3
                k = first * (i + 1) + (1 - first) * f
                lev = ((k - 2) * (k - 3) // 2) * f1 + ((k - 1) * (3 - k)) * f2 + ((k - 1) * (k - 2) // 2) * f3
                dx = (1 - first) * (1 - i % 2)
                dy = (1 - first) * ((i + 1) // 2)
                yy = y + dy - 2 * y * dy
                xx = x + dx - 2 * x * dx
                sids = (shard_of(lev, yy, xx, c), shard_of(lev, yy, xx, 1 - c))
                row0 = pl.multiple_of(i * sh.pair, sh.pair)
                rows.load(sids)
                rows.select(sids)

                @pl.when(i == 0)
                def _():
                    await_weights(weights, w, w_sem)

                rows.forward(row0)
                rows.finish(row0)
                return carry

            lax.fori_loop(0, 3, body, None)

        for step in (1, 2):

            @pl.when(f == step)
            def _():
                theirs(step)

        pl.run_scoped(rows_phase, *row_scratch(sh))

        def tick(it):
            @pl.when(jnp.logical_and(f == 0, it == blocks * 5 // 6))
            def _():
                stage(1)

            @pl.when(jnp.logical_and(f == 1, it == blocks // 2))
            def _():
                stage(2)

        def grads_phase(*vm):
            add_weight_grads(sh, 3 * sh.pair, hbm, grads, put_stacked(grads), vm, grad_sems, tick)

        pl.run_scoped(grads_phase, *grad_scratch(sh, 3 * sh.pair))
        return carry

    lax.fori_loop(0, 3, group, None)
    stage(3)
    theirs(3)
    links.drain()


def third_kernel(sh, xb, gb, mb, grads, w1, w3, w2, out1, out3, out2, xs_h, do_h, d_h, w_sem, in_sem, out_sem, *grad_sems):
    z, e, y, x, c = where_am_i()
    bufs, weights = (xb, gb, mb), (w1, w3, w2)
    lev = other_levels(z)[2]
    hbm = (xs_h, do_h, d_h)

    def rows_phase(w, stage_v, meta, xs, do, a, d1, d3):
        load_weights(weights, w, w_sem)
        rows = Rows(sh, e, bufs, None, w, (stage_v, meta, xs, do, a, d1, d3), (in_sem, out_sem), hbm)

        def body(i, carry):
            dx = 1 - i % 2
            dy = (i + 1) // 2
            yy = y + dy - 2 * y * dy
            xx = x + dx - 2 * x * dx
            sids = (shard_of(lev, yy, xx, c), shard_of(lev, yy, xx, 1 - c))
            row0 = pl.multiple_of(i * sh.pair, sh.pair)
            rows.load(sids)
            rows.select(sids)

            @pl.when(i == 0)
            def _():
                await_weights(weights, w, w_sem)

            rows.forward(row0)
            rows.finish(row0)
            return carry

        lax.fori_loop(0, 3, body, None)

    pl.run_scoped(rows_phase, *row_scratch(sh))

    def grads_phase(*vm):
        add_weight_grads(sh, 3 * sh.pair, hbm, grads, put_separate((out1, out3, out2)), vm, grad_sems)

    pl.run_scoped(grads_phase, *grad_scratch(sh, 3 * sh.pair))


def cost(sh, shards, products):
    return pl.CostEstimate(flops=2 * shards * sh.cap * sh.d * sh.f * products, bytes_accessed=300_000_000, transcendentals=0)


def solution(mesh):
    tok_spec = P(("dp", "ep"), None)
    exp_spec = P("ep", None, None)

    def device_step(x_loc, route_idx, w_router, w_gate, w_up, w_down, dy_loc):
        t, top_k = route_idx.shape
        d = x_loc.shape[1]
        n_exp = w_router.shape[1]
        f = w_down.shape[1]
        cap = 3 * t * top_k // n_exp
        sh = Shapes(t, d, f, cap)
        w1, w3, w2 = jnp.swapaxes(w_gate[0], 0, 1), jnp.swapaxes(w_up[0], 0, 1), w_down[0]

        logits = jnp.dot(x_loc, w_router, preferred_element_type=F32)
        experts = jnp.arange(n_exp, dtype=jnp.int32)
        chose = (route_idx[:, :, None] == experts).astype(F32)
        gate_probs = jax.nn.softmax(jnp.sum(chose * logits[:, None, :], axis=2), axis=-1)
        chose_any = jnp.sum(chose, axis=1)
        before = (jnp.arange(t)[:, None] > jnp.arange(t)[None, :]).astype(BF)
        rank = jnp.dot(before, chose_any.astype(BF), preferred_element_type=F32)
        pos = jnp.where(chose_any > 0, rank, NOWHERE)
        gate = jnp.sum(chose * gate_probs[:, :, None], axis=1)
        meta = jnp.concatenate([pos.T, gate.T], axis=0)
        slot = jnp.sum(chose * rank[:, None, :], axis=2).astype(jnp.int32)

        shape = jax.ShapeDtypeStruct
        gathered = [shape((32, t, d), BF), shape((32, t, d), BF), shape((32, 16, t), F32)]
        grads_shape = shape((3, f, d), F32)

        def row_shapes(pairs):
            n = pairs * sh.pair
            return [shape((n, d), BF), shape((n, d), BF), shape((3, n, f), BF)]

        outs = pl.pallas_call(
            functools.partial(first_kernel, sh),
            out_shape=gathered + [shape((n_exp, cap, d), BF), shape((n_exp, 8, sh.pair), F32), shape((8, cap, d), BF), shape((8, 8, sh.pair), F32)]
            + row_shapes(4) + [grads_shape],
            in_specs=[ANY] * 6,
            out_specs=[ANY] * 11,
            scratch_shapes=[pltpu.SemaphoreType.DMA((24, 3)), pltpu.SemaphoreType.DMA((32, 3)), pltpu.SemaphoreType.DMA((8, 2)), pltpu.SemaphoreType.DMA((8, 2))]
            + ROW_SEMS + [pltpu.SemaphoreType.DMA((4,))] + GRAD_SEMS,
            compiler_params=pltpu.CompilerParams(collective_id=0, has_side_effects=True, vmem_limit_bytes=VMEM_LIMIT),
            cost_estimate=cost(sh, 8, 9),
            name="own_level",
        )(x_loc, dy_loc, meta, w1, w3, w2)
        xb, gb, mb, rback, qback = outs[:5]
        grads = outs[-1]

        xb, gb, mb, grads = pl.pallas_call(
            functools.partial(second_kernel, sh),
            out_shape=gathered + [grads_shape] + row_shapes(3),
            in_specs=[ANY] * 7,
            out_specs=[ANY] * 7,
            input_output_aliases={0: 0, 1: 1, 2: 2, 3: 3},
            scratch_shapes=[pltpu.SemaphoreType.DMA((28, 3)), pltpu.SemaphoreType.DMA((32, 3))] + ROW_SEMS + GRAD_SEMS,
            compiler_params=pltpu.CompilerParams(collective_id=1, has_side_effects=True, vmem_limit_bytes=VMEM_LIMIT),
            cost_estimate=cost(sh, 18, 6),
            name="other_levels",
        )(xb, gb, mb, grads, w1, w3, w2)[:4]

        g1, g3, g2 = pl.pallas_call(
            functools.partial(third_kernel, sh),
            out_shape=[shape((f, d), F32)] * 3 + row_shapes(3),
            in_specs=[ANY] * 7,
            out_specs=[ANY] * 6,
            scratch_shapes=ROW_SEMS + GRAD_SEMS,
            compiler_params=pltpu.CompilerParams(vmem_limit_bytes=VMEM_LIMIT),
            cost_estimate=cost(sh, 6, 6),
            name="last_level",
        )(xb, gb, mb, grads, w1, w3, w2)[:3]

        at = route_idx * cap + slot
        dx_choice = rback.reshape(n_exp * cap, d)[at.reshape(-1)].reshape(t, top_k, d)
        q_half = qback[:, 0, :].reshape(n_exp, 2, cap)
        same = (experts % 2 == lax.axis_index("ep") % 2)[:, None]
        q_slot = jnp.where(same, q_half[:, 0], q_half[:, 1])
        hit = rank[:, :, None] == jnp.arange(cap, dtype=F32)
        q_tok = jnp.sum(jnp.where(hit, q_slot[None], 0.0), axis=2)
        dgate = jnp.sum(chose * q_tok[:, None, :], axis=2)
        d_sel = gate_probs * (dgate - jnp.sum(gate_probs * dgate, axis=1, keepdims=True))
        d_logits = jnp.sum(chose * d_sel[:, :, None], axis=1).astype(BF)
        du_router = lax.dot_general(d_logits, w_router, NT, preferred_element_type=F32)
        grad_router = lax.dot_general(x_loc, d_logits, TN, preferred_element_type=F32)
        grad_router = lax.psum(grad_router, ("dp", "ep"))
        grad_x = (jnp.sum(dx_choice.astype(F32), axis=1) + du_router).astype(BF)
        return grad_x, jnp.swapaxes(g1, 0, 1)[None], jnp.swapaxes(g3, 0, 1)[None], g2[None], grad_router

    return jax.shard_map(
        device_step, mesh=mesh, in_specs=(tok_spec, tok_spec, P(), exp_spec, exp_spec, exp_spec, tok_spec),
        out_specs=(tok_spec, exp_spec, exp_spec, exp_spec, P()), check_vma=False)
```

```python
import functools

import jax
import jax.numpy as jnp
from jax import lax
from jax.experimental import pallas as pl
from jax.experimental.pallas import tpu as pltpu
from jax.sharding import PartitionSpec as P

BF = jnp.bfloat16
F32 = jnp.float32
MESH = pl.DeviceIdType.MESH
ANY = pl.BlockSpec(memory_space=pl.ANY)
NT = (((1,), (1,)), ((), ()))
TN = (((0,), (0,)), ((), ()))
NN = (((1,), (0,)), ((), ()))
TT = (((0,), (1,)), ((), ()))
VMEM_LIMIT = 67_000_000
NOWHERE = 300.0


def mm(left, right, dims=NN):
    return lax.dot_general(left, right, dims, preferred_element_type=F32)


def where_am_i():
    z = lax.axis_index("dp")
    e = lax.axis_index("ep")
    return z, e, e // 4, (e // 2) % 2, e % 2


def shard_of(z, y, x, c):
    return z * 8 + y * 4 + x * 2 + c


def other_levels(z):
    return z + 1 - 2 * (z % 2), 2 - z // 2, 3 - 3 * (z // 2)


class Shapes:
    def __init__(self, tokens, width, hidden, cap):
        self.t, self.d, self.f, self.cap = tokens, width, hidden, cap
        self.pair = 2 * cap
        self.wide = min(512, width)
        self.whole = hidden // 256 * 256
        self.tail = hidden - self.whole
        half = (self.whole // 2 + 255) // 256 * 256
        self.cuts = [(lo, hi) for lo, hi in ((0, half), (half, self.whole)) if lo < hi]


def rows_of(sh, half):
    return slice(half * sh.cap, (half + 1) * sh.cap)


class Links:
    def __init__(self, bufs, own, ssem, rsem, partner):
        self.bufs, self.own, self.ssem, self.rsem, self.partner = bufs, own, ssem, rsem, partner
        self.sent = {}

    def _copy(self, slot, part, sid, dev, own):
        src = self.own[part] if own else self.bufs[part].at[sid]
        return pltpu.make_async_remote_copy(
            src_ref=src,
            dst_ref=self.bufs[part].at[sid],
            send_sem=self.ssem.at[slot, part],
            recv_sem=self.rsem.at[sid, part],
            device_id=dev,
            device_id_type=MESH,
        )

    def _do(self, when, go):
        if when is None:
            go()
        else:
            pl.when(when())(go)

    def send(self, tag, sid, dev, parts=(0, 1, 2), when=None, own=False):
        if tag not in self.sent:
            self.sent[tag] = (len(self.sent), sid, dev, parts, when, own)
        slot = self.sent[tag][0]

        def go():
            for part in parts:
                self._copy(slot, part, sid(), dev, own).start()

        self._do(when, go)

    def arrived(self, sid, parts=(0, 1, 2), when=None):
        def go():
            for part in parts:
                self._copy(0, part, sid(), self.partner, False).wait_recv()

        self._do(when, go)

    def drain(self):
        for slot, sid, dev, parts, when, own in self.sent.values():

            def go():
                for part in parts:
                    self._copy(slot, part, sid(), dev, own).wait_send()

            self._do(when, go)

    def along_column(self, name, step, z, shard, above, below, where=None):
        ends = (lambda: z % 3 == 0)
        for side, sid, exists, onward, on_exists in (
            ("top", lambda: shard(z + step), lambda: z + step <= 3, below, lambda: z > 0),
            ("bottom", lambda: shard(z - step), lambda: z >= step, above, lambda: z < 3),
        ):

            def when(exists=exists):
                if where is None:
                    return exists()
                level = ends() if where == "ends" else jnp.logical_not(ends())
                return jnp.logical_and(exists(), level)

            self.arrived(sid, when=when)
            if step < 3 and where != "ends":
                self.send((name, step, side, where, "on"), sid, onward, when=lambda when=when, on=on_exists: jnp.logical_and(when(), on()))
            self.send((name, step, side, where, "partner"), sid, self.partner, when=when)


def enter(peers):
    barrier = pltpu.get_barrier_semaphore()
    for dev in peers:
        pl.semaphore_signal(barrier, device_id=dev, device_id_type=MESH)
    pl.semaphore_wait(barrier, len(peers))


def pick_rows(sh, half, stage, meta, expert, xs, do, gs):
    cap, t, wide = sh.cap, sh.t, sh.wide
    pos = meta[half, pl.ds(expert, 1), :]
    gate = meta[half, pl.ds(8 + expert, 1), :]
    slot = lax.broadcasted_iota(jnp.int32, (cap, t), 0).astype(F32)
    hit = slot == pos
    pick = jnp.where(hit, 1.0, 0.0).astype(BF)
    gate_col = jnp.sum(jnp.where(hit, gate, 0.0), axis=1, keepdims=True)
    rows = rows_of(sh, half)
    for n in range(0, sh.d, wide):
        cols = slice(n, n + wide)
        xs[rows, cols] = mm(pick, stage[2 * half, :, cols]).astype(BF)
        g_sel = mm(pick, stage[2 * half + 1, :, cols])
        do[rows, cols] = (gate_col * g_sel).astype(BF)
        gs[rows, cols] = g_sel.astype(BF)


def expert_rows(sh, w, w_tail, xs, do, a, d1, d3):
    def put(cols, z1, z3):
        da = mm(do[...], w[2, cols, :], NT)
        sig = jax.nn.sigmoid(z1)
        silu = z1 * sig
        a[:, cols] = (silu * z3).astype(BF)
        d1[:, cols] = (da * z3 * sig * (1.0 + z1 * (1.0 - sig))).astype(BF)
        d3[:, cols] = (da * silu).astype(BF)

    for lo, hi in sh.cuts:
        cols = slice(lo, hi)
        put(cols, mm(xs[...], w[0, cols, :], NT), mm(xs[...], w[1, cols, :], NT))
    both = mm(xs[...], w_tail[...], NT)
    put(slice(sh.whole, sh.f), both[:, : sh.tail], both[:, sh.tail :])


def token_rows(sh, w, a, d1, d3, gs, kept, qt):
    acc = jnp.zeros((sh.pair, 1), F32)
    for n in range(0, sh.d, sh.wide):
        cols = slice(n, n + sh.wide)
        out = mm(a[...], w[2, :, cols])
        acc = acc + jnp.sum(out * gs[:, cols].astype(F32), axis=1, keepdims=True)
    slot = lax.broadcasted_iota(jnp.int32, (sh.cap, sh.t), 0).astype(F32)
    for half in range(2):
        q = jnp.where(slot == kept[half, 0:1, :], acc[rows_of(sh, half), :], 0.0)
        qt[half] = jnp.broadcast_to(jnp.sum(q, axis=0, keepdims=True), (8, sh.t))
    for n in range(0, sh.d, sh.wide):
        cols = slice(n, n + sh.wide)
        row = mm(d1[...], w[0, :, cols]) + mm(d3[...], w[1, :, cols])
        gs[:, cols] = row.astype(BF)


class Rows:
    def __init__(self, sh, expert, bufs, own, w, vm, sems, hbm):
        self.sh, self.expert, self.bufs, self.own, self.w = sh, expert, bufs, own, w
        self.stage, self.meta, self.xs, self.do, self.a, self.d1, self.d3 = vm
        self.in_sem, self.out_sem = sems
        self.xs_h, self.do_h, self.d_h = hbm

    def _in(self, half, part, sid, own=False):
        src = self.own[part] if own else self.bufs[part].at[sid]
        dst = self.meta.at[half] if part == 2 else self.stage.at[2 * half + part]
        return pltpu.make_async_copy(src, dst, self.in_sem.at[half, part])

    def load(self, sids, own_first=False):
        for half in range(2):
            for part in (2, 0, 1):
                self._in(half, part, sids[half], own_first and half == 0).start()

    def select(self, sids, gs, kept):
        for half in range(2):
            for part in (2, 0, 1):
                self._in(half, part, sids[half]).wait()
            pick_rows(self.sh, half, self.stage, self.meta, self.expert, self.xs, self.do, gs)
            kept[half] = jnp.broadcast_to(self.meta[half, pl.ds(self.expert, 1), :], (8, self.sh.t))

    def out(self, k, row0):
        at = pl.ds(row0, self.sh.pair)
        src = (self.xs, self.do, self.d1, self.d3, self.a)[k]
        dst = (self.xs_h, self.do_h)[k].at[at, :] if k < 2 else self.d_h.at[k - 2, at, :]
        return pltpu.make_async_copy(src, dst, self.out_sem.at[k])

    def start_outs(self, row0, which):
        for k in which:
            self.out(k, row0).start()

    def wait_outs(self, row0, which):
        for k in which:
            self.out(k, row0).wait()


def add_weight_grads(sh, rows, hbm, grad_in, put, vm, sems, tick=None, fresh=None):
    xs_h, do_h, d_h = hbm
    d_v, y_v, acc = vm
    d_sem, y_sem, i_sem, o_sem = sems
    nblk = sh.d // sh.wide
    total = 3 * nblk
    ny, na = y_v.shape[0], acc.shape[0]

    def column(it):
        return pl.multiple_of((it % nblk) * sh.wide, sh.wide)

    def d_copy(k):
        return pltpu.make_async_copy(d_h.at[k, pl.ds(0, rows), :], d_v.at[k % 2], d_sem.at[k % 2])

    def y_copy(it, src):
        return pltpu.make_async_copy(src.at[pl.ds(0, rows), pl.ds(column(it), sh.wide)], y_v.at[it % ny], y_sem.at[it % ny])

    def acc_copy(it):
        return pltpu.make_async_copy(grad_in.at[it // nblk, :, pl.ds(column(it), sh.wide)], acc.at[it % na], i_sem.at[it % na])

    def acc_out(it, start):
        put(it // nblk, column(it), acc.at[it % na], o_sem.at[it % na], start)

    def fetch_y(it):
        @pl.when(it < 2 * nblk)
        def _():
            y_copy(it, xs_h).start()

        @pl.when(it >= 2 * nblk)
        def _():
            y_copy(it, do_h).start()

    def fetch_acc(it):
        if fresh is None:
            acc_copy(it).start()
        else:

            @pl.when(jnp.logical_not(fresh))
            def _():
                acc_copy(it).start()

    d_copy(0).start()
    fetch_y(0)
    fetch_acc(0)
    fetch_acc(1)

    def body(it, carry):
        k = it // nblk

        @pl.when(it % nblk == 0)
        def _():
            @pl.when(k < 2)
            def _():
                d_copy(k + 1).start()

            d_copy(k).wait()

        @pl.when(it >= 2)
        def _():
            acc_out(it - 2, False)

        @pl.when(it + 1 < total)
        def _():
            fetch_y(it + 1)

        @pl.when(it + 2 < total)
        def _():
            fetch_acc(it + 2)

        if tick is not None:
            tick(it)
        y_copy(it, xs_h).wait()

        def products(add):
            for lo in range(0, sh.f, sh.wide):
                at = slice(lo, min(lo + sh.wide, sh.f))
                new = mm(d_v[k % 2, :, at], y_v[it % ny], TN)
                acc[it % na, at, :] = acc[it % na, at, :] + new if add else new

        def add_products():
            acc_copy(it).wait()
            products(True)

        if fresh is None:
            add_products()
        else:
            pl.when(fresh)(lambda: products(False))
            pl.when(jnp.logical_not(fresh))(add_products)
        acc_out(it, True)
        return carry

    lax.fori_loop(0, total, body, None)
    acc_out(total - 2, False)
    acc_out(total - 1, False)


def put_stacked(grads):
    def put(k, col, src, sem, start):
        copy = pltpu.make_async_copy(src, grads.at[k, :, pl.ds(col, src.shape[-1])], sem)
        copy.start() if start else copy.wait()

    return put


def put_separate(grads):
    def put(k, col, src, sem, start):
        if start:
            for j in range(3):

                @pl.when(k == j)
                def _():
                    pltpu.make_async_copy(src, grads[j].at[:, pl.ds(col, src.shape[-1])], sem).start()
        else:
            pltpu.make_async_copy(src, grads[0].at[:, pl.ds(col, src.shape[-1])], sem).wait()

    return put


def row_scratch(sh):
    return (
        pltpu.VMEM((4, sh.t, sh.d), BF),
        pltpu.VMEM((2, 16, sh.t), F32),
        pltpu.VMEM((sh.pair, sh.d), BF),
        pltpu.VMEM((sh.pair, sh.d), BF),
        pltpu.VMEM((sh.pair, sh.f), BF),
        pltpu.VMEM((sh.pair, sh.f), BF),
        pltpu.VMEM((sh.pair, sh.f), BF),
    )


def grad_scratch(sh, rows):
    return (
        pltpu.VMEM((2, rows, sh.f), BF),
        pltpu.VMEM((2, rows, sh.wide), BF),
        pltpu.VMEM((4, sh.f, sh.wide), F32),
    )


GRAD_SEMS = [pltpu.SemaphoreType.DMA((2,)), pltpu.SemaphoreType.DMA((2,)), pltpu.SemaphoreType.DMA((4,)), pltpu.SemaphoreType.DMA((4,))]
ROW_SEMS = [pltpu.SemaphoreType.DMA((5,)), pltpu.SemaphoreType.DMA((2, 3)), pltpu.SemaphoreType.DMA((5,))]


def main_kernel(sh, x_in, g_in, m_in, w1, w3, w2, xb, gb, mb, rback, qback, r_h, q_h, xs_h, do_h, d_h, grads, router, w, w_tail,
                total, parts, q_v, m_v, ssem, rsem, ret_s, ret_r, sum_s, sum_r, sum_l, w_sem, in_sem, out_sem, loc_sem, *grad_sems):
    z, e, y, x, c = where_am_i()
    me = shard_of(z, y, x, c)
    bufs, own, weights = (xb, gb, mb), (x_in, g_in, m_in), (w1, w3, w2)
    partner, xn, yn = (z, e + 1 - 2 * c), (z, e + 2 - 4 * x), (z, e + 4 - 8 * y)
    above, below = (z + 1, e), (z - 1, e)
    links = Links(bufs, own, ssem, rsem, partner)
    levels = (z, *other_levels(z))
    columns = [(y, x), (y, 1 - x), (1 - y, x), (1 - y, 1 - x)]
    O, X, Y, D = range(4)
    places = " ".join(("O0 X0 Y0 O1", "D0 O2 X1 Y1", "D1 X2 Y2 O3", "D2 X3 Y3 D3")).split()
    order = [("OXYD".index(chip), int(level)) for chip, level in places]
    plane = [(z, yy * 4 + xx * 2 + cc) for yy, xx in columns for cc in (c, 1 - c)]

    def mine(col, k):
        return shard_of(levels[k], *columns[col], c)

    def theirs(col, k):
        return shard_of(levels[k], *columns[col], 1 - c)

    enter(plane[1:] + [((z + j) % 4, e) for j in (1, 2, 3)])
    links.send("p", lambda: me, partner, own=True)
    links.send("x", lambda: me, xn, own=True)
    links.send("y", lambda: me, yn, own=True)
    links.send("u", lambda: me, above, when=lambda: z < 3, own=True)
    links.send("d", lambda: me, below, when=lambda: z > 0, own=True)

    def column(name, step, where=None):
        col = O if name == "o" else D
        links.along_column(name, step, z, lambda lev: shard_of(lev, *columns[col], c), above, below, where)

    def sideways(k):
        links.send(("x", k), lambda: mine(O, k), xn)
        links.send(("y", k), lambda: mine(O, k), yn)

    def sides_in(k):
        for col in (X, Y):
            links.arrived(lambda: mine(col, k))
            links.send((col, k, "partner"), lambda col=col: mine(col, k), partner)

    def ret(k, part):
        src, dst = ((r_h, rback), (q_h, qback))[part]
        return pltpu.make_async_remote_copy(
            src_ref=src.at[k], dst_ref=dst.at[e], send_sem=ret_s.at[k, part], recv_sem=ret_r.at[e, part],
            device_id=plane[k], device_id_type=MESH)

    def ret_in(k, part):
        src, dst = ((r_h, rback), (q_h, qback))[part]
        peer = plane[k][1]
        return pltpu.make_async_remote_copy(
            src_ref=src.at[k], dst_ref=dst.at[peer], send_sem=ret_s.at[k, part], recv_sem=ret_r.at[peer, part],
            device_id=plane[k], device_id_type=MESH)

    def send_back(places, part=0):
        for k in places:
            ret(k, part).start()

    def hop(k):
        return pltpu.make_async_remote_copy(
            src_ref=total, dst_ref=parts.at[k], send_sem=sum_s.at[k], recv_sem=sum_r.at[k],
            device_id=(partner, xn, yn)[k], device_id_type=MESH)

    def level_hop(j):
        return pltpu.make_async_remote_copy(
            src_ref=total, dst_ref=parts.at[3 + z], send_sem=sum_s.at[2 + j], recv_sem=sum_r.at[3 + z],
            device_id=((z + j) % 4, e), device_id_type=MESH)

    def level_in(j):
        lev = (z + j) % 4
        return pltpu.make_async_remote_copy(
            src_ref=total, dst_ref=parts.at[3 + lev], send_sem=sum_s.at[2 + j], recv_sem=sum_r.at[3 + lev],
            device_id=(lev, e), device_id_type=MESH)

    def router_part(rows):
        for k in range(1, 8):
            ret_in(k, 1).wait_recv()
        x_rows = rows.at[0 : sh.t, :]
        copies = [pltpu.make_async_copy(src, dst, sum_l.at[k]) for k, (src, dst) in enumerate(((qback, q_v), (m_in, m_v), (x_in, x_rows)))]
        for copy in copies:
            copy.start()
        for copy in copies:
            copy.wait()
        gate, q = m_v[8:16, :], q_v[:, 0, :]
        d_sel = gate * (q - jnp.sum(gate * q, axis=0, keepdims=True))
        d_logits = d_sel.astype(BF)
        for n in range(0, sh.d, sh.wide):
            cols = slice(n, n + sh.wide)
            total[:, cols] = mm(d_logits, rows[0 : sh.t, cols])

    def add_hop(k):
        hop(k).wait()
        total[...] += parts[k]

    def before(n, rows):
        if n == 1:
            links.arrived(lambda: mine(X, 0))
            links.send("xy", lambda: mine(X, 0), yn, parts=(1,))
            links.arrived(lambda: mine(Y, 0))
            links.send("yx", lambda: mine(Y, 0), xn, parts=(0, 2))
            links.send("xp", lambda: mine(X, 0), partner)
            links.send("yp", lambda: mine(Y, 0), partner)
            column("o", 1)
            sideways(1)
        if n == 3:
            links.arrived(lambda: mine(D, 0))
            links.send("dp", lambda: mine(D, 0), partner)
            links.send("du", lambda: mine(D, 0), above, when=lambda: z < 3)
            links.send("dd", lambda: mine(D, 0), below, when=lambda: z > 0)
            send_back((1, 2, 3), part=1)
        if n == 4:
            send_back((4, 5), part=1)
        if n == 5:
            column("d", 1)
            router_part(rows)
            hop(0).start()
        if n == 6:
            add_hop(0)
            hop(1).start()
            send_back(range(1, 6))
        if n == 7:
            add_hop(1)
            hop(2).start()
        if n == 8:
            sides_in(2)
        if n == 9:
            column("o", 3)
            sideways(3)
        if n == 10:
            add_hop(2)
            for j in (1, 2, 3):
                level_hop(j).start()
            parts[3 + z] = total[...]
        if n == 12:
            column("d", 2, "ends")
        if n == 13:
            sides_in(3)
        if n == 15:
            column("d", 3)

    def during(g, it):
        if g == 0 and it == 1:
            send_back((6, 7), part=1)
            column("o", 2)
            sideways(2)
        if g == 0 and it == 12:
            sides_in(1)
        if g == 1 and it == 1:
            column("d", 2, "middle")
        if g == 1 and it == 4:
            send_back((6, 7))

    def pick(table, n):
        low, high = sum(v * 4**i for i, v in enumerate(table[:10])), sum(v * 4**i for i, v in enumerate(table[10:]))
        in_high = n // 10
        word = low * (1 - in_high) + high * in_high
        return lax.shift_right_logical(word, 2 * (n - 10 * in_high)) % 4

    def sids_of(n):
        col, k = pick([a for a, _ in order], n), pick([b for _, b in order], n)
        dx, dy = col % 2, col // 2
        yy, xx = y + dy - 2 * y * dy, x + dx - 2 * x * dx
        f1, f2, f3 = levels[1:]
        lev = (
            ((1 - k) * (2 - k) * (3 - k) // 6) * z
            + (k * (2 - k) * (3 - k) // 2) * f1
            + (k * (k - 1) * (3 - k) // 2) * f2
            + (k * (k - 1) * (k - 2) // 6) * f3
        )
        return shard_of(lev, yy, xx, c), shard_of(lev, yy, xx, 1 - c)

    ahead = (2, 3, 4, 6, 7, 8, 9, 11, 14)
    tail = pl.ds(sh.whole, sh.tail)
    weights_in = lambda: [pltpu.make_async_copy(weights[k], w.at[k], w_sem.at[k]) for k in range(3)] + [
        pltpu.make_async_copy(weights[k].at[tail, :], w_tail.at[pl.ds(k * sh.tail, sh.tail), :], w_sem.at[3 + k]) for k in range(2)
    ]
    for copy in weights_in():
        copy.start()
    blocks = 3 * (sh.d // sh.wide)

    def group(g, carry):
        def rows_phase(stage, meta, xs, do, a, d1, d3, gs, kept, qt):
            rows = Rows(sh, e, bufs, own, w, (stage, meta, xs, do, a, d1, d3), (in_sem, out_sem), (xs_h, do_h, d_h))

            def keep(n, start):
                for half in range(2):
                    at = rows_of(sh, half)
                    copies = lambda r, q: (
                        pltpu.make_async_copy(gs.at[at, :], r, loc_sem.at[half]),
                        pltpu.make_async_copy(qt.at[half], q, loc_sem.at[2 + half]),
                    )
                    place = n_place(n) * 2 + half
                    if not start:
                        for copy in copies(r_h.at[place], q_h.at[place]):
                            copy.wait()
                        continue


                    def go(r, q):
                        for copy in copies(r, q):
                            copy.start()

                    pl.when(place == 0)(lambda: go(rback.at[e], qback.at[e]))
                    pl.when(place > 0)(lambda: go(r_h.at[place], q_h.at[place]))

            def n_place(n):
                return n - n // 4

            def body(i, carry):
                pl.when(i < 5 + g // 2)(lambda: one_pair(i))
                return carry

            def one_pair(i):
                n = g * 5 + i
                sids, row0 = sids_of(n), pl.multiple_of(i * sh.pair, sh.pair)
                own_level = jnp.logical_and(n < 5, n != 3)
                for k in range(16):

                    @pl.when(n == k)
                    def _():
                        before(k, gs)
                        if k not in ahead:
                            links.arrived(lambda: theirs(*order[k]))
                            rows.load(sids, own_first=k == 0)

                @pl.when(i > 0)
                def _():
                    rows.wait_outs(row0, (0, 1))

                @pl.when(jnp.logical_and(n > 0, n < 4))
                def _():
                    keep(n - 1, False)

                rows.select(sids, gs, kept)
                rows.start_outs(row0, (0, 1))
                for k in ahead:

                    @pl.when(n + 1 == k)
                    def _():
                        links.arrived(lambda: theirs(*order[k]))
                        rows.load(sids_of(n + 1))

                @pl.when(n == 0)
                def _():
                    for copy in weights_in():
                        copy.wait()

                @pl.when(i > 0)
                def _():
                    rows.wait_outs(row0, (2, 3, 4))

                expert_rows(sh, w, w_tail, xs, do, a, d1, d3)
                rows.start_outs(row0, (2, 3, 4))

                @pl.when(own_level)
                def _():
                    token_rows(sh, w, a, d1, d3, gs, kept, qt)
                    keep(n, True)

                @pl.when(n == 4)
                def _():
                    keep(n, False)

            lax.fori_loop(0, 6, body, None)
            rows.wait_outs(0, range(5))

        pl.run_scoped(rows_phase, *row_scratch(sh), pltpu.VMEM((sh.pair, sh.d), BF), pltpu.VMEM((2, 8, sh.t), F32),
                      pltpu.VMEM((2, 8, sh.t), F32))

        def tick(it):
            for gg, when in ((0, 1), (0, 12), (1, 1), (1, 4)):

                @pl.when(jnp.logical_and(g == gg, it == when * blocks // 24))
                def _():
                    during(gg, when)

        @pl.when(g < 2)
        def _():
            def grads_phase(*vm):
                add_weight_grads(sh, 5 * sh.pair, (xs_h, do_h, d_h), grads, put_stacked(grads), vm, grad_sems, tick, g == 0)

            pl.run_scoped(grads_phase, *grad_scratch(sh, 5 * sh.pair))

        return carry

    lax.fori_loop(0, 3, group, None)
    for j in (1, 2, 3):
        level_hop(j).wait_send()
        level_in(j).wait_recv()
    total[...] = ((parts[3] + parts[4]) + parts[5]) + parts[6]
    copy = pltpu.make_async_copy(total, router, sum_l.at[0])
    copy.start()
    for k in range(1, 8):
        ret(k, 0).wait_send()
        ret(k, 1).wait_send()
        ret_in(k, 0).wait_recv()
    copy.wait()
    links.drain()


def last_kernel(sh, grads, xs_h, do_h, d_h, out1, out3, out2, *sems):
    def grads_phase(*vm):
        add_weight_grads(sh, 6 * sh.pair, (xs_h, do_h, d_h), grads, put_separate((out1, out3, out2)), vm, sems)

    pl.run_scoped(grads_phase, *grad_scratch(sh, 6 * sh.pair))


def cost(sh, shards, products):
    return pl.CostEstimate(flops=2 * shards * sh.cap * sh.d * sh.f * products, bytes_accessed=300_000_000, transcendentals=0)


def solution(mesh):
    tok_spec = P(("dp", "ep"), None)
    exp_spec = P("ep", None, None)

    def device_step(x_loc, route_idx, w_router, w_gate, w_up, w_down, dy_loc):
        t, top_k = route_idx.shape
        d = x_loc.shape[1]
        n_exp = w_router.shape[1]
        f = w_down.shape[1]
        cap = 3 * t * top_k // n_exp
        sh = Shapes(t, d, f, cap)
        w1, w3, w2 = jnp.swapaxes(w_gate[0], 0, 1), jnp.swapaxes(w_up[0], 0, 1), w_down[0]

        chosen = route_idx.T
        experts = jnp.arange(n_exp, dtype=jnp.int32)
        logits = mm(w_router, x_loc, TT)
        chose = (chosen[:, None, :] == experts[None, :, None]).astype(F32)
        gate_probs = jax.nn.softmax(jnp.sum(chose * logits[None], axis=1), axis=0)
        chose_any = jnp.sum(chose, axis=0)
        before = (jnp.arange(t)[:, None] < jnp.arange(t)[None, :]).astype(BF)
        rank = jnp.dot(chose_any.astype(BF), before, preferred_element_type=F32)
        pos = jnp.where(chose_any > 0, rank, NOWHERE)
        gate = jnp.sum(chose * gate_probs[:, None, :], axis=0)
        meta = jnp.concatenate([pos, gate], axis=0)

        shape = jax.ShapeDtypeStruct
        gathered = [shape((32, t, d), BF), shape((32, t, d), BF), shape((32, 16, t), F32)]
        n = 6 * sh.pair
        row_shapes = [shape((n, d), BF), shape((n, d), BF), shape((3, n, f), BF)]
        weights_vmem = pltpu.VMEM((3, f, d), BF)

        outs = pl.pallas_call(
            functools.partial(main_kernel, sh),
            out_shape=gathered + [shape((n_exp, cap, d), BF), shape((n_exp, 8, t), F32), shape((8, cap, d), BF), shape((8, 8, t), F32)]
            + row_shapes + [shape((3, f, d), F32), shape((n_exp, d), F32)],
            in_specs=[ANY] * 6,
            out_specs=[ANY] * 12,
            scratch_shapes=[weights_vmem, pltpu.VMEM((2 * sh.tail, d), BF), pltpu.VMEM((n_exp, d), F32), pltpu.VMEM((7, n_exp, d), F32), pltpu.VMEM((n_exp, 8, t), F32), pltpu.VMEM((16, t), F32), pltpu.SemaphoreType.DMA((48, 3)), pltpu.SemaphoreType.DMA((32, 3)), pltpu.SemaphoreType.DMA((8, 2)), pltpu.SemaphoreType.DMA((8, 2)),
                pltpu.SemaphoreType.DMA((6,)), pltpu.SemaphoreType.DMA((7,)), pltpu.SemaphoreType.DMA((3,))]
            + ROW_SEMS + [pltpu.SemaphoreType.DMA((4,))] + GRAD_SEMS,
            compiler_params=pltpu.CompilerParams(collective_id=0, has_side_effects=True, vmem_limit_bytes=VMEM_LIMIT),
            cost_estimate=cost(sh, 32, 5),
            name="gather_and_rows",
        )(x_loc, dy_loc, meta, w1, w3, w2)
        rback, qback, _, _, xs_h, do_h, d_h, grads, router = outs[3:]

        g1, g3, g2 = pl.pallas_call(
            functools.partial(last_kernel, sh),
            out_shape=[shape((f, d), F32)] * 3,
            in_specs=[ANY] * 4,
            out_specs=[ANY] * 3,
            scratch_shapes=GRAD_SEMS,
            compiler_params=pltpu.CompilerParams(vmem_limit_bytes=VMEM_LIMIT),
            cost_estimate=cost(sh, 12, 3),
            name="last_weight_grads",
        )(grads, xs_h, do_h, d_h)

        dgate = jnp.sum(chose * qback[None, :, 0, :], axis=1)
        d_sel = gate_probs * (dgate - jnp.sum(gate_probs * dgate, axis=0, keepdims=True))
        d_logits = jnp.sum(chose * d_sel[:, None, :], axis=0).astype(BF)
        du_router = mm(d_logits, w_router, TT)
        hit = (pos[:, None, :] == jnp.arange(cap, dtype=F32)[None, :, None]).astype(BF).reshape(n_exp * cap, t)
        rows_sum = mm(hit, rback.reshape(n_exp * cap, d), TN)
        grad_x = (rows_sum + du_router).astype(BF)
        return grad_x, jnp.swapaxes(g1, 0, 1)[None], jnp.swapaxes(g3, 0, 1)[None], g2[None], router.T

    return jax.shard_map(
        device_step, mesh=mesh, in_specs=(tok_spec, tok_spec, P(), exp_spec, exp_spec, exp_spec, tok_spec),
        out_specs=(tok_spec, exp_spec, exp_spec, exp_spec, P()), check_vma=False)
```

```python
import functools

import jax
import jax.numpy as jnp
from jax import lax
from jax.experimental import pallas as pl
from jax.experimental.pallas import tpu as pltpu
from jax.sharding import PartitionSpec as P

BF = jnp.bfloat16
F32 = jnp.float32
MESH = pl.DeviceIdType.MESH
ANY = pl.BlockSpec(memory_space=pl.ANY)
NT = (((1,), (1,)), ((), ()))
TN = (((0,), (0,)), ((), ()))
NN = (((1,), (0,)), ((), ()))
TT = (((0,), (1,)), ((), ()))
VMEM_LIMIT = 67_000_000
NOWHERE = 300.0


def mm(left, right, dims=NN):
    return lax.dot_general(left, right, dims, preferred_element_type=F32)


def where_am_i():
    z = lax.axis_index("dp")
    e = lax.axis_index("ep")
    return z, e, e // 4, (e // 2) % 2, e % 2


def shard_of(z, y, x, c):
    return z * 8 + y * 4 + x * 2 + c


def other_levels(z):
    return z + 1 - 2 * (z % 2), 2 - z // 2, 3 - 3 * (z // 2)


class Shapes:
    def __init__(self, tokens, width, hidden, cap):
        self.t, self.d, self.f, self.cap = tokens, width, hidden, cap
        self.pair = 2 * cap
        self.wide = min(512, width)
        self.whole = hidden // 256 * 256
        self.tail = hidden - self.whole
        half = (self.whole // 2 + 255) // 256 * 256
        self.cuts = [(lo, hi) for lo, hi in ((0, half), (half, self.whole)) if lo < hi]


def rows_of(sh, half):
    return slice(half * sh.cap, (half + 1) * sh.cap)


class Links:
    def __init__(self, bufs, own, ssem, rsem, partner):
        self.bufs, self.own, self.ssem, self.rsem, self.partner = bufs, own, ssem, rsem, partner
        self.sent = {}

    def _copy(self, slot, part, sid, dev, own):
        src = self.own[part] if own else self.bufs[part].at[sid]
        return pltpu.make_async_remote_copy(
            src_ref=src,
            dst_ref=self.bufs[part].at[sid],
            send_sem=self.ssem.at[slot, part],
            recv_sem=self.rsem.at[sid, part],
            device_id=dev,
            device_id_type=MESH,
        )

    def _do(self, when, go):
        if when is None:
            go()
        else:
            pl.when(when())(go)

    def send(self, tag, sid, dev, parts=(0, 1, 2), when=None, own=False):
        if tag not in self.sent:
            self.sent[tag] = (len(self.sent), sid, dev, parts, when, own)
        slot = self.sent[tag][0]

        def go():
            for part in parts:
                self._copy(slot, part, sid(), dev, own).start()

        self._do(when, go)

    def arrived(self, sid, parts=(0, 1, 2), when=None):
        def go():
            for part in parts:
                self._copy(0, part, sid(), self.partner, False).wait_recv()

        self._do(when, go)

    def drain(self):
        for slot, sid, dev, parts, when, own in self.sent.values():

            def go():
                for part in parts:
                    self._copy(slot, part, sid(), dev, own).wait_send()

            self._do(when, go)

    def along_column(self, name, step, z, shard, above, below, where=None):
        ends = (lambda: z % 3 == 0)
        for side, sid, exists, onward, on_exists in (
            ("top", lambda: shard(z + step), lambda: z + step <= 3, below, lambda: z > 0),
            ("bottom", lambda: shard(z - step), lambda: z >= step, above, lambda: z < 3),
        ):

            def when(exists=exists):
                if where is None:
                    return exists()
                level = ends() if where == "ends" else jnp.logical_not(ends())
                return jnp.logical_and(exists(), level)

            self.arrived(sid, when=when)
            if step < 3 and where != "ends":
                self.send((name, step, side, where, "on"), sid, onward, when=lambda when=when, on=on_exists: jnp.logical_and(when(), on()))
            self.send((name, step, side, where, "partner"), sid, self.partner, when=when)


def enter(peers):
    barrier = pltpu.get_barrier_semaphore()
    for dev in peers:
        pl.semaphore_signal(barrier, device_id=dev, device_id_type=MESH)
    pl.semaphore_wait(barrier, len(peers))


def pick_rows(sh, half, stage, meta, expert, xs, do, gs):
    cap, t, wide = sh.cap, sh.t, sh.wide
    pos = meta[half, pl.ds(expert, 1), :]
    gate = meta[half, pl.ds(8 + expert, 1), :]
    slot = lax.broadcasted_iota(jnp.int32, (cap, t), 0).astype(F32)
    hit = slot == pos
    pick = jnp.where(hit, 1.0, 0.0).astype(BF)
    gate_col = jnp.sum(jnp.where(hit, gate, 0.0), axis=1, keepdims=True)
    rows = rows_of(sh, half)
    for n in range(0, sh.d, wide):
        cols = slice(n, n + wide)
        xs[rows, cols] = mm(pick, stage[2 * half, :, cols]).astype(BF)
        g_sel = mm(pick, stage[2 * half + 1, :, cols])
        do[rows, cols] = (gate_col * g_sel).astype(BF)
        gs[rows, cols] = g_sel.astype(BF)


def expert_rows(sh, w, w_tail, xs, do, a, d1, d3):
    def put(cols, z1, z3):
        da = mm(do[...], w[2, cols, :], NT)
        sig = jax.nn.sigmoid(z1)
        silu = z1 * sig
        a[:, cols] = (silu * z3).astype(BF)
        d1[:, cols] = (da * z3 * sig * (1.0 + z1 * (1.0 - sig))).astype(BF)
        d3[:, cols] = (da * silu).astype(BF)

    for lo, hi in sh.cuts:
        cols = slice(lo, hi)
        put(cols, mm(xs[...], w[0, cols, :], NT), mm(xs[...], w[1, cols, :], NT))
    both = mm(xs[...], w_tail[...], NT)
    put(slice(sh.whole, sh.f), both[:, : sh.tail], both[:, sh.tail :])


def token_rows(sh, w, a, d1, d3, gs, kept, qt):
    acc = jnp.zeros((sh.pair, 1), F32)
    for n in range(0, sh.d, sh.wide):
        cols = slice(n, n + sh.wide)
        out = mm(a[...], w[2, :, cols])
        acc = acc + jnp.sum(out * gs[:, cols].astype(F32), axis=1, keepdims=True)
    slot = lax.broadcasted_iota(jnp.int32, (sh.cap, sh.t), 0).astype(F32)
    for half in range(2):
        q = jnp.where(slot == kept[half, 0:1, :], acc[rows_of(sh, half), :], 0.0)
        qt[half] = jnp.broadcast_to(jnp.sum(q, axis=0, keepdims=True), (8, sh.t))
    for n in range(0, sh.d, sh.wide):
        cols = slice(n, n + sh.wide)
        row = mm(d1[...], w[0, :, cols]) + mm(d3[...], w[1, :, cols])
        gs[:, cols] = row.astype(BF)


class Rows:
    def __init__(self, sh, expert, bufs, own, w, vm, sems, hbm):
        self.sh, self.expert, self.bufs, self.own, self.w = sh, expert, bufs, own, w
        self.stage, self.meta, self.xs, self.do, self.a, self.d1, self.d3 = vm
        self.in_sem, self.out_sem = sems
        self.xs_h, self.do_h, self.d_h = hbm

    def _in(self, half, part, sid, own=False):
        src = self.own[part] if own else self.bufs[part].at[sid]
        dst = self.meta.at[half] if part == 2 else self.stage.at[2 * half + part]
        return pltpu.make_async_copy(src, dst, self.in_sem.at[half, part])

    def load(self, sids, own_first=False):
        for half in range(2):
            for part in (2, 0, 1):
                self._in(half, part, sids[half], own_first and half == 0).start()

    def select(self, sids, gs, kept):
        for half in range(2):
            for part in (2, 0, 1):
                self._in(half, part, sids[half]).wait()
            pick_rows(self.sh, half, self.stage, self.meta, self.expert, self.xs, self.do, gs)
            kept[half] = jnp.broadcast_to(self.meta[half, pl.ds(self.expert, 1), :], (8, self.sh.t))

    def out(self, k, row0):
        at = pl.ds(row0, self.sh.pair)
        src = (self.xs, self.do, self.d1, self.d3, self.a)[k]
        dst = (self.xs_h, self.do_h)[k].at[at, :] if k < 2 else self.d_h.at[k - 2, at, :]
        return pltpu.make_async_copy(src, dst, self.out_sem.at[k])

    def start_outs(self, row0, which):
        for k in which:
            self.out(k, row0).start()

    def wait_outs(self, row0, which):
        for k in which:
            self.out(k, row0).wait()


def add_weight_grads(sh, rows, hbm, grad_in, put, vm, sems, tick=None, fresh=None):
    xs_h, do_h, d_h = hbm
    d_v, y_v, acc = vm
    d_sem, y_sem, i_sem, o_sem = sems
    wide = y_v.shape[-1]
    nblk = sh.d // wide
    total = 3 * nblk
    ny, na = y_v.shape[0], acc.shape[0]

    def column(it):
        return pl.multiple_of((it % nblk) * wide, wide)

    def d_copy(k):
        return pltpu.make_async_copy(d_h.at[k, pl.ds(0, rows), :], d_v.at[k % 2], d_sem.at[k % 2])

    def y_copy(it, src):
        return pltpu.make_async_copy(src.at[pl.ds(0, rows), pl.ds(column(it), wide)], y_v.at[it % ny], y_sem.at[it % ny])

    def acc_copy(it):
        return pltpu.make_async_copy(grad_in.at[it // nblk, :, pl.ds(column(it), wide)], acc.at[it % na], i_sem.at[it % na])

    def acc_out(it, start):
        put(it // nblk, column(it), acc.at[it % na], o_sem.at[it % na], start)

    def fetch_y(it):
        @pl.when(it < 2 * nblk)
        def _():
            y_copy(it, xs_h).start()

        @pl.when(it >= 2 * nblk)
        def _():
            y_copy(it, do_h).start()

    def fetch_acc(it):
        if fresh is None:
            acc_copy(it).start()
        else:

            @pl.when(jnp.logical_not(fresh))
            def _():
                acc_copy(it).start()

    d_copy(0).start()
    fetch_y(0)
    fetch_acc(0)
    fetch_acc(1)

    def body(it, carry):
        k = it // nblk

        @pl.when(it % nblk == 0)
        def _():
            @pl.when(k < 2)
            def _():
                d_copy(k + 1).start()

            d_copy(k).wait()

        @pl.when(it >= 2)
        def _():
            acc_out(it - 2, False)

        @pl.when(it + 1 < total)
        def _():
            fetch_y(it + 1)

        @pl.when(it + 2 < total)
        def _():
            fetch_acc(it + 2)

        if tick is not None:
            tick(it)
        y_copy(it, xs_h).wait()

        def products(add):
            for lo in range(0, sh.f, wide):
                at = slice(lo, min(lo + wide, sh.f))
                new = mm(d_v[k % 2, :, at], y_v[it % ny], TN)
                acc[it % na, at, :] = acc[it % na, at, :] + new if add else new

        def add_products():
            acc_copy(it).wait()
            products(True)

        if fresh is None:
            add_products()
        else:
            pl.when(fresh)(lambda: products(False))
            pl.when(jnp.logical_not(fresh))(add_products)
        acc_out(it, True)
        return carry

    lax.fori_loop(0, total, body, None)
    acc_out(total - 2, False)
    acc_out(total - 1, False)


def put_stacked(grads):
    def put(k, col, src, sem, start):
        copy = pltpu.make_async_copy(src, grads.at[k, :, pl.ds(col, src.shape[-1])], sem)
        copy.start() if start else copy.wait()

    return put


def put_separate(grads):
    def put(k, col, src, sem, start):
        if start:
            for j in range(3):

                @pl.when(k == j)
                def _():
                    pltpu.make_async_copy(src, grads[j].at[:, pl.ds(col, src.shape[-1])], sem).start()
        else:
            pltpu.make_async_copy(src, grads[0].at[:, pl.ds(col, src.shape[-1])], sem).wait()

    return put


def row_scratch(sh):
    return (
        pltpu.VMEM((4, sh.t, sh.d), BF),
        pltpu.VMEM((2, 16, sh.t), F32),
        pltpu.VMEM((sh.pair, sh.d), BF),
        pltpu.VMEM((sh.pair, sh.d), BF),
        pltpu.VMEM((sh.pair, sh.f), BF),
        pltpu.VMEM((sh.pair, sh.f), BF),
        pltpu.VMEM((sh.pair, sh.f), BF),
    )


def grad_scratch(sh, rows, wide):
    return (
        pltpu.VMEM((2, rows, sh.f), BF),
        pltpu.VMEM((2, rows, wide), BF),
        pltpu.VMEM((4, sh.f, wide), F32),
    )


GRAD_SEMS = [pltpu.SemaphoreType.DMA((2,)), pltpu.SemaphoreType.DMA((2,)), pltpu.SemaphoreType.DMA((4,)), pltpu.SemaphoreType.DMA((4,))]
ROW_SEMS = [pltpu.SemaphoreType.DMA((5,)), pltpu.SemaphoreType.DMA((2, 3)), pltpu.SemaphoreType.DMA((5,))]


def main_kernel(sh, x_in, g_in, m_in, w1, w3, w2, xb, gb, mb, rback, qback, r_h, q_h, xs_h, do_h, d_h, grads, router, w, w_tail,
                total, parts, q_v, m_v, ssem, rsem, ret_s, ret_r, sum_s, sum_r, sum_l, w_sem, in_sem, out_sem, loc_sem, *grad_sems):
    z, e, y, x, c = where_am_i()
    me = shard_of(z, y, x, c)
    bufs, own, weights = (xb, gb, mb), (x_in, g_in, m_in), (w1, w3, w2)
    partner, xn, yn = (z, e + 1 - 2 * c), (z, e + 2 - 4 * x), (z, e + 4 - 8 * y)
    above, below = (z + 1, e), (z - 1, e)
    links = Links(bufs, own, ssem, rsem, partner)
    levels = (z, *other_levels(z))
    columns = [(y, x), (y, 1 - x), (1 - y, x), (1 - y, 1 - x)]
    O, X, Y, D = range(4)
    places = " ".join(("O0 X0 Y0 O1", "D0 O2 X1 Y1", "D1 X2 Y2 O3", "D2 X3 Y3 D3")).split()
    order = [("OXYD".index(chip), int(level)) for chip, level in places]
    plane = [(z, yy * 4 + xx * 2 + cc) for yy, xx in columns for cc in (c, 1 - c)]

    def mine(col, k):
        return shard_of(levels[k], *columns[col], c)

    def theirs(col, k):
        return shard_of(levels[k], *columns[col], 1 - c)

    enter(plane[1:] + [((z + j) % 4, e) for j in (1, 2, 3)])
    links.send("p", lambda: me, partner, own=True)
    links.send("x", lambda: me, xn, own=True)
    links.send("y", lambda: me, yn, own=True)
    links.send("u", lambda: me, above, when=lambda: z < 3, own=True)
    links.send("d", lambda: me, below, when=lambda: z > 0, own=True)

    def column(name, step, where=None):
        col = O if name == "o" else D
        links.along_column(name, step, z, lambda lev: shard_of(lev, *columns[col], c), above, below, where)

    def sideways(k):
        links.send(("x", k), lambda: mine(O, k), xn)
        links.send(("y", k), lambda: mine(O, k), yn)

    def sides_in(k):
        for col in (X, Y):
            links.arrived(lambda: mine(col, k))
            links.send((col, k, "partner"), lambda col=col: mine(col, k), partner)

    def ret(k, part):
        src, dst = ((r_h, rback), (q_h, qback))[part]
        return pltpu.make_async_remote_copy(
            src_ref=src.at[k], dst_ref=dst.at[e], send_sem=ret_s.at[k, part], recv_sem=ret_r.at[e, part],
            device_id=plane[k], device_id_type=MESH)

    def ret_in(k, part):
        src, dst = ((r_h, rback), (q_h, qback))[part]
        peer = plane[k][1]
        return pltpu.make_async_remote_copy(
            src_ref=src.at[k], dst_ref=dst.at[peer], send_sem=ret_s.at[k, part], recv_sem=ret_r.at[peer, part],
            device_id=plane[k], device_id_type=MESH)

    def send_back(places, part=0):
        for k in places:
            ret(k, part).start()

    def hop(k):
        return pltpu.make_async_remote_copy(
            src_ref=total, dst_ref=parts.at[k], send_sem=sum_s.at[k], recv_sem=sum_r.at[k],
            device_id=(partner, xn, yn)[k], device_id_type=MESH)

    def level_hop(j):
        return pltpu.make_async_remote_copy(
            src_ref=total, dst_ref=parts.at[3 + z], send_sem=sum_s.at[2 + j], recv_sem=sum_r.at[3 + z],
            device_id=((z + j) % 4, e), device_id_type=MESH)

    def level_in(j):
        lev = (z + j) % 4
        return pltpu.make_async_remote_copy(
            src_ref=total, dst_ref=parts.at[3 + lev], send_sem=sum_s.at[2 + j], recv_sem=sum_r.at[3 + lev],
            device_id=(lev, e), device_id_type=MESH)

    def router_part(rows):
        for k in range(1, 8):
            ret_in(k, 1).wait_recv()
        x_rows = rows.at[0 : sh.t, :]
        copies = [pltpu.make_async_copy(src, dst, sum_l.at[k]) for k, (src, dst) in enumerate(((qback, q_v), (m_in, m_v), (x_in, x_rows)))]
        for copy in copies:
            copy.start()
        for copy in copies:
            copy.wait()
        gate, q = m_v[8:16, :], q_v[:, 0, :]
        d_sel = gate * (q - jnp.sum(gate * q, axis=0, keepdims=True))
        d_logits = d_sel.astype(BF)
        for n in range(0, sh.d, sh.wide):
            cols = slice(n, n + sh.wide)
            total[:, cols] = mm(d_logits, rows[0 : sh.t, cols])

    def add_hop(k):
        hop(k).wait()
        total[...] += parts[k]

    def before(n, rows):
        if n == 1:
            links.arrived(lambda: mine(X, 0))
            links.send("xy", lambda: mine(X, 0), yn, parts=(1,))
            links.arrived(lambda: mine(Y, 0))
            links.send("yx", lambda: mine(Y, 0), xn, parts=(0, 2))
            links.send("xp", lambda: mine(X, 0), partner)
            links.send("yp", lambda: mine(Y, 0), partner)
            column("o", 1)
            sideways(1)
        if n == 3:
            links.arrived(lambda: mine(D, 0))
            links.send("dp", lambda: mine(D, 0), partner)
            links.send("du", lambda: mine(D, 0), above, when=lambda: z < 3)
            links.send("dd", lambda: mine(D, 0), below, when=lambda: z > 0)
            send_back((1, 2, 3), part=1)
        if n == 4:
            send_back((4, 5), part=1)
        if n == 5:
            column("d", 1)
            router_part(rows)
            hop(0).start()
        if n == 6:
            add_hop(0)
            hop(1).start()
            send_back(range(1, 6))
        if n == 7:
            add_hop(1)
            hop(2).start()
        if n == 8:
            sides_in(2)
        if n == 9:
            column("o", 3)
            sideways(3)
        if n == 10:
            add_hop(2)
            for j in (1, 2, 3):
                level_hop(j).start()
            parts[3 + z] = total[...]
        if n == 12:
            column("d", 2, "ends")
        if n == 13:
            sides_in(3)
        if n == 15:
            column("d", 3)

    def during(g, it):
        if g == 0 and it == 1:
            send_back((6, 7), part=1)
            column("o", 2)
            sideways(2)
        if g == 0 and it == 12:
            sides_in(1)
        if g == 1 and it == 1:
            column("d", 2, "middle")
        if g == 1 and it == 4:
            send_back((6, 7))

    def pick(table, n):
        low, high = sum(v * 4**i for i, v in enumerate(table[:10])), sum(v * 4**i for i, v in enumerate(table[10:]))
        in_high = n // 10
        word = low * (1 - in_high) + high * in_high
        return lax.shift_right_logical(word, 2 * (n - 10 * in_high)) % 4

    def sids_of(n):
        col, k = pick([a for a, _ in order], n), pick([b for _, b in order], n)
        dx, dy = col % 2, col // 2
        yy, xx = y + dy - 2 * y * dy, x + dx - 2 * x * dx
        f1, f2, f3 = levels[1:]
        lev = (
            ((1 - k) * (2 - k) * (3 - k) // 6) * z
            + (k * (2 - k) * (3 - k) // 2) * f1
            + (k * (k - 1) * (3 - k) // 2) * f2
            + (k * (k - 1) * (k - 2) // 6) * f3
        )
        return shard_of(lev, yy, xx, c), shard_of(lev, yy, xx, 1 - c)

    ahead = (2, 3, 4, 6, 7, 8, 9, 11, 14)
    tail = pl.ds(sh.whole, sh.tail)
    weights_in = lambda: [pltpu.make_async_copy(weights[k], w.at[k], w_sem.at[k]) for k in range(3)] + [
        pltpu.make_async_copy(weights[k].at[tail, :], w_tail.at[pl.ds(k * sh.tail, sh.tail), :], w_sem.at[3 + k]) for k in range(2)
    ]
    for copy in weights_in():
        copy.start()
    blocks = 3 * (sh.d // sh.wide)

    def group(g, carry):
        def rows_phase(stage, meta, xs, do, a, d1, d3, gs, kept, qt):
            rows = Rows(sh, e, bufs, own, w, (stage, meta, xs, do, a, d1, d3), (in_sem, out_sem), (xs_h, do_h, d_h))

            def keep(n, start):
                for half in range(2):
                    at = rows_of(sh, half)
                    copies = lambda r, q: (
                        pltpu.make_async_copy(gs.at[at, :], r, loc_sem.at[half]),
                        pltpu.make_async_copy(qt.at[half], q, loc_sem.at[2 + half]),
                    )
                    place = n_place(n) * 2 + half
                    if not start:
                        for copy in copies(r_h.at[place], q_h.at[place]):
                            copy.wait()
                        continue


                    def go(r, q):
                        for copy in copies(r, q):
                            copy.start()

                    pl.when(place == 0)(lambda: go(rback.at[e], qback.at[e]))
                    pl.when(place > 0)(lambda: go(r_h.at[place], q_h.at[place]))

            def n_place(n):
                return n - n // 4

            def body(i, carry):
                pl.when(i < 5 + g // 2)(lambda: one_pair(i))
                return carry

            def one_pair(i):
                n = g * 5 + i
                sids, row0 = sids_of(n), pl.multiple_of(i * sh.pair, sh.pair)
                own_level = jnp.logical_and(n < 5, n != 3)
                for k in range(16):

                    @pl.when(n == k)
                    def _():
                        before(k, gs)
                        if k not in ahead:
                            links.arrived(lambda: theirs(*order[k]))
                            rows.load(sids, own_first=k == 0)

                @pl.when(i > 0)
                def _():
                    rows.wait_outs(row0, (0, 1))

                @pl.when(jnp.logical_and(n > 0, n < 4))
                def _():
                    keep(n - 1, False)

                rows.select(sids, gs, kept)
                rows.start_outs(row0, (0, 1))
                for k in ahead:

                    @pl.when(n + 1 == k)
                    def _():
                        links.arrived(lambda: theirs(*order[k]))
                        rows.load(sids_of(n + 1))

                @pl.when(n == 0)
                def _():
                    for copy in weights_in():
                        copy.wait()

                @pl.when(i > 0)
                def _():
                    rows.wait_outs(row0, (2, 3, 4))

                expert_rows(sh, w, w_tail, xs, do, a, d1, d3)
                rows.start_outs(row0, (2, 3, 4))

                @pl.when(own_level)
                def _():
                    token_rows(sh, w, a, d1, d3, gs, kept, qt)
                    keep(n, True)

                @pl.when(n == 4)
                def _():
                    keep(n, False)

            lax.fori_loop(0, 6, body, None)
            rows.wait_outs(0, range(5))

        pl.run_scoped(rows_phase, *row_scratch(sh), pltpu.VMEM((sh.pair, sh.d), BF), pltpu.VMEM((2, 8, sh.t), F32),
                      pltpu.VMEM((2, 8, sh.t), F32))

        def tick(it):
            for gg, when in ((0, 1), (0, 12), (1, 1), (1, 4)):

                @pl.when(jnp.logical_and(g == gg, it == when * blocks // 24))
                def _():
                    during(gg, when)

        @pl.when(g < 2)
        def _():
            def grads_phase(*vm):
                add_weight_grads(sh, 5 * sh.pair, (xs_h, do_h, d_h), grads, put_stacked(grads), vm, grad_sems, tick, g == 0)

            pl.run_scoped(grads_phase, *grad_scratch(sh, 5 * sh.pair, sh.wide))

        return carry

    lax.fori_loop(0, 3, group, None)
    for j in (1, 2, 3):
        level_hop(j).wait_send()
        level_in(j).wait_recv()
    total[...] = ((parts[3] + parts[4]) + parts[5]) + parts[6]
    copy = pltpu.make_async_copy(total, router, sum_l.at[0])
    copy.start()
    for k in range(1, 8):
        ret(k, 0).wait_send()
        ret(k, 1).wait_send()
        ret_in(k, 0).wait_recv()
    copy.wait()
    links.drain()


def last_kernel(sh, grads, xs_h, do_h, d_h, out1, out3, out2, *sems):
    def grads_phase(*vm):
        add_weight_grads(sh, 6 * sh.pair, (xs_h, do_h, d_h), grads, put_separate((out1, out3, out2)), vm, sems)

    pl.run_scoped(grads_phase, *grad_scratch(sh, 6 * sh.pair, min(2 * sh.wide, sh.d)))


def cost(sh, shards, products):
    return pl.CostEstimate(flops=2 * shards * sh.cap * sh.d * sh.f * products, bytes_accessed=300_000_000, transcendentals=0)


def solution(mesh):
    tok_spec = P(("dp", "ep"), None)
    exp_spec = P("ep", None, None)

    def device_step(x_loc, route_idx, w_router, w_gate, w_up, w_down, dy_loc):
        t, top_k = route_idx.shape
        d = x_loc.shape[1]
        n_exp = w_router.shape[1]
        f = w_down.shape[1]
        cap = 3 * t * top_k // n_exp
        sh = Shapes(t, d, f, cap)
        w1, w3, w2 = jnp.swapaxes(w_gate[0], 0, 1), jnp.swapaxes(w_up[0], 0, 1), w_down[0]

        chosen = route_idx.T
        experts = jnp.arange(n_exp, dtype=jnp.int32)
        logits = mm(w_router, x_loc, TT)
        chose = (chosen[:, None, :] == experts[None, :, None]).astype(F32)
        gate_probs = jax.nn.softmax(jnp.sum(chose * logits[None], axis=1), axis=0)
        chose_any = jnp.sum(chose, axis=0)
        before = (jnp.arange(t)[:, None] < jnp.arange(t)[None, :]).astype(BF)
        rank = jnp.dot(chose_any.astype(BF), before, preferred_element_type=F32)
        pos = jnp.where(chose_any > 0, rank, NOWHERE)
        gate = jnp.sum(chose * gate_probs[:, None, :], axis=0)
        meta = jnp.concatenate([pos, gate], axis=0)

        shape = jax.ShapeDtypeStruct
        gathered = [shape((32, t, d), BF), shape((32, t, d), BF), shape((32, 16, t), F32)]
        n = 6 * sh.pair
        row_shapes = [shape((n, d), BF), shape((n, d), BF), shape((3, n, f), BF)]
        weights_vmem = pltpu.VMEM((3, f, d), BF)

        outs = pl.pallas_call(
            functools.partial(main_kernel, sh),
            out_shape=gathered + [shape((n_exp, cap, d), BF), shape((n_exp, 8, t), F32), shape((8, cap, d), BF), shape((8, 8, t), F32)]
            + row_shapes + [shape((3, f, d), F32), shape((n_exp, d), F32)],
            in_specs=[ANY] * 6,
            out_specs=[ANY] * 12,
            scratch_shapes=[weights_vmem, pltpu.VMEM((2 * sh.tail, d), BF), pltpu.VMEM((n_exp, d), F32), pltpu.VMEM((7, n_exp, d), F32), pltpu.VMEM((n_exp, 8, t), F32), pltpu.VMEM((16, t), F32), pltpu.SemaphoreType.DMA((48, 3)), pltpu.SemaphoreType.DMA((32, 3)), pltpu.SemaphoreType.DMA((8, 2)), pltpu.SemaphoreType.DMA((8, 2)),
                pltpu.SemaphoreType.DMA((6,)), pltpu.SemaphoreType.DMA((7,)), pltpu.SemaphoreType.DMA((3,))]
            + ROW_SEMS + [pltpu.SemaphoreType.DMA((4,))] + GRAD_SEMS,
            compiler_params=pltpu.CompilerParams(collective_id=0, has_side_effects=True, vmem_limit_bytes=VMEM_LIMIT),
            cost_estimate=cost(sh, 32, 5),
            name="gather_and_rows",
        )(x_loc, dy_loc, meta, w1, w3, w2)
        rback, qback, _, _, xs_h, do_h, d_h, grads, router = outs[3:]

        g1, g3, g2 = pl.pallas_call(
            functools.partial(last_kernel, sh),
            out_shape=[shape((f, d), F32)] * 3,
            in_specs=[ANY] * 4,
            out_specs=[ANY] * 3,
            scratch_shapes=GRAD_SEMS,
            compiler_params=pltpu.CompilerParams(vmem_limit_bytes=VMEM_LIMIT),
            cost_estimate=cost(sh, 12, 3),
            name="last_weight_grads",
        )(grads, xs_h, do_h, d_h)

        dgate = jnp.sum(chose * qback[None, :, 0, :], axis=1)
        d_sel = gate_probs * (dgate - jnp.sum(gate_probs * dgate, axis=0, keepdims=True))
        d_logits = jnp.sum(chose * d_sel[:, None, :], axis=0).astype(BF)
        du_router = mm(d_logits, w_router, TT)
        hit = (pos[:, None, :] == jnp.arange(cap, dtype=F32)[None, :, None]).astype(BF).reshape(n_exp * cap, t)
        rows_sum = mm(hit, rback.reshape(n_exp * cap, d), TN)
        grad_x = (rows_sum + du_router).astype(BF)
        return grad_x, jnp.swapaxes(g1, 0, 1)[None], jnp.swapaxes(g3, 0, 1)[None], g2[None], router.T

    return jax.shard_map(
        device_step, mesh=mesh, in_specs=(tok_spec, tok_spec, P(), exp_spec, exp_spec, exp_spec, tok_spec),
        out_specs=(tok_spec, exp_spec, exp_spec, exp_spec, P()), check_vma=False)
```
